128 devices in a mesh: depth: 4 (over z), col: 4 (over y), row: 8 (over x, core).
Axes of the slice: x: 4, y: 4, z: 4, core: 2. Of those that a mesh axis runs over, the one named last changes fastest.
Arguments:
- a_mat: bfloat16 [12288, 12288], P('row', 'col')
- b_mat: bfloat16 [12288, 12288], P('row', 'col')
Outputs:
- output: bfloat16 [12288, 12288], P(('row', 'depth'), 'col')
All inputs are finite; a program needn't handle non-finite values.
Results may differ from the reference program's by a relative error of at most 0.001.
Values are sent between devices in bfloat16 or wider.
A program may use at most 1 GiB of HBM per device.

```python
import jax
import jax.numpy as jnp

D = 12288


def setup_inputs(seed: int = 0) -> dict:
    key_a, key_b = jax.random.split(jax.random.key(seed))
    a_mat = jax.random.normal(key_a, (D, D), jnp.float32) + 0.5
    b_mat = (jax.random.normal(key_b, (D, D), jnp.float32) + 2.0 * D ** -0.5) * D ** -0.5
    return {"a_mat": a_mat.astype(jnp.bfloat16), "b_mat": b_mat.astype(jnp.bfloat16)}


def reference(a_mat, b_mat):
    return jnp.dot(a_mat, b_mat, preferred_element_type=jnp.float32).astype(jnp.bfloat16)
```

```python
import functools

import jax
import jax.numpy as jnp
from jax import lax
from jax.experimental import pallas as pl
from jax.experimental.pallas import tpu as pltpu
from jax.sharding import PartitionSpec as P

MESH = pl.DeviceIdType.MESH

A_OWN, A_FWD, A_Z = 0, 4, 6
B_OWN, B_FWD, B_Z, B_D2D = 9, 11, 13, 16
KINDS = 20
LAG = 4


def kernel(steps, seg, a_ref, b_ref, c_ref, a_buf, b_buf, acc, c_st, snd, rcv, loc, c_snd, c_rcv, c_loc):
    band, kblk = a_ref.shape
    half_m, half_n = band // 2, kblk // 2
    third_m, third_n = half_m // 3, half_n // 3
    l = lax.axis_index("depth")
    y = lax.axis_index("col")
    i = lax.axis_index("row")
    x, c = i // 2, lax.rem(i, 2)
    h, e = l // 2, lax.rem(l, 2)
    n = lax.rem((l + 1) // 2, 2)
    role_a, role_b = e, h
    yp, ym, y2 = lax.rem(y + 1, 4), lax.rem(y + 3, 4), lax.rem(y + 2, 4)
    xp, xm, x2 = lax.rem(x + 1, 4), lax.rem(x + 3, 4), lax.rem(x + 2, 4)
    dev_yp, dev_ym = {"col": yp}, {"col": ym}
    dev_xp, dev_xm = {"row": 2 * xp + c}, {"row": 2 * xm + c}
    dev_za, dev_zb = {"depth": l + 1 - 2 * e}, {"depth": 3 - l}
    dev_sib = {"row": i + 1 - 2 * c}

    def al(v, m=128):
        return pl.multiple_of(v, m)

    def remote(kind, q, src, dst, dev):
        return pltpu.make_async_remote_copy(
            src_ref=src, dst_ref=dst, send_sem=snd.at[kind, q], recv_sem=rcv.at[kind, q], device_id=dev, device_id_type=MESH
        )

    def a_own(q):
        out = []
        for d, dev in enumerate((dev_yp, dev_ym)):
            for p in range(2):
                src = a_ref.at[pl.ds(al(h * half_m + third_m * role_a), 2 * third_m), pl.ds(al(p * band + q * seg), seg)]
                dst = a_buf.at[q, pl.ds(al(third_m * role_a), 2 * third_m), pl.ds(al((2 * y + p) * seg), seg)]
                out.append(remote(A_OWN + 2 * d + p, q, src, dst, dev))
        return out

    def a_fwd(q):
        out = []
        for d, (blk, dev) in enumerate(((ym, dev_yp), (yp, dev_ym))):
            ref = a_buf.at[q, pl.ds(al(third_m * (role_a + d)), third_m), pl.ds(al(2 * blk * seg), 2 * seg)]
            out.append(remote(A_FWD + d, q, ref, ref, dev))
        return out

    def a_z(q, which):
        blk = (ym, yp, y2)[which]
        ref = a_buf.at[q, pl.ds(al(2 * third_m * role_a), third_m), pl.ds(al(2 * blk * seg), 2 * seg)]
        return remote(A_Z + which, q, ref, ref, dev_za)

    def b_own(q):
        out = []
        for d, dev in enumerate((dev_xp, dev_xm)):
            src = b_ref.at[pl.ds(al(q * seg), seg), pl.ds(al(n * half_n + third_n * role_b), 2 * third_n)]
            dst = b_buf.at[q, pl.ds(al((2 * x + c) * seg), seg), pl.ds(al(third_n * role_b), 2 * third_n)]
            out.append(remote(B_OWN + d, q, src, dst, dev))
        return out

    def b_fwd(q):
        out = []
        for d, (blk, dev) in enumerate(((xm, dev_xp), (xp, dev_xm))):
            ref = b_buf.at[q, pl.ds(al((2 * blk + c) * seg), seg), pl.ds(al(third_n * (role_b + d)), third_n)]
            out.append(remote(B_FWD + d, q, ref, ref, dev))
        return out

    def b_z(q, which):
        blk = (xm, xp, x2)[which]
        ref = b_buf.at[q, pl.ds(al((2 * blk + c) * seg), seg), pl.ds(al(2 * third_n * role_b), third_n)]
        return remote(B_Z + which, q, ref, ref, dev_zb)

    def b_d2d(q, which):
        blk = (xm, xp, x2, x)[which]
        dst = b_buf.at[q, pl.ds(al((2 * blk + c) * seg), seg), :]
        src = b_ref.at[pl.ds(al(q * seg), seg), pl.ds(al(n * half_n), half_n)] if which == 3 else dst
        return remote(B_D2D + which, q, src, dst, dev_sib)

    def local(q):
        out = []
        for p in range(2):
            src = a_ref.at[pl.ds(al(h * half_m), half_m), pl.ds(al(p * band + q * seg), seg)]
            dst = a_buf.at[q, :, pl.ds(al((2 * y + p) * seg), seg)]
            out.append(pltpu.make_async_copy(src, dst, loc.at[p, q]))
        src = b_ref.at[pl.ds(al(q * seg), seg), pl.ds(al(n * half_n), half_n)]
        dst = b_buf.at[q, pl.ds(al((2 * x + c) * seg), seg), :]
        out.append(pltpu.make_async_copy(src, dst, loc.at[2, q]))
        return out

    barrier = pltpu.get_barrier_semaphore()
    partners = (dev_yp, dev_ym, dev_xp, dev_xm, dev_za, dev_zb, dev_sib)
    for dev in partners:
        pl.semaphore_signal(barrier, inc=1, device_id=dev, device_id_type=MESH)
    pl.semaphore_wait(barrier, len(partners))

    tile_n = third_n

    def zero_tile(r, _):
        acc[pl.ds(al(r * 64, 64), 64), :] = jnp.zeros((64, half_n), jnp.float32)
        return 0

    def wait_inputs(q):
        for cp in local(q):
            cp.wait()
        for which in range(3):
            a_z(q, which).wait_recv()
        for which in range(4):
            b_d2d(q, which).wait_recv()

    def send_own(q):
        for cp in b_own(q) + a_own(q) + [b_d2d(q, 3)] + local(q):
            cp.start()

    def first_hop(q):
        for cp in b_own(q):
            cp.wait_recv()
        for cp in b_fwd(q) + [b_z(q, 0), b_z(q, 1)]:
            cp.start()
        for cp in a_own(q):
            cp.wait_recv()
        for cp in a_fwd(q) + [a_z(q, 0), a_z(q, 1)]:
            cp.start()

    def second_hop(q):
        for cp in b_fwd(q):
            cp.wait_recv()
        b_z(q, 2).start()
        for cp in a_fwd(q):
            cp.wait_recv()
        a_z(q, 2).start()
        for which in range(2):
            b_z(q, which).wait_recv()
            b_d2d(q, which).start()

    def last_hop(q):
        b_z(q, 2).wait_recv()
        b_d2d(q, 2).start()

    def compute(q):
        wait_inputs(q)

        def tile(j, _):
            rows = pl.ds(al((j // 3) * third_m), third_m)
            cols = pl.ds(al(lax.rem(j, 3) * tile_n), tile_n)
            acc[rows, cols] += jnp.dot(a_buf[q, rows, :], b_buf[q, :, cols], preferred_element_type=jnp.float32)
            return 0

        lax.fori_loop(0, 9, tile, 0)

    def body(t, _):
        pl.when(t < steps)(lambda: send_own(t))

        @pl.when(t == 0)
        def _():
            lax.fori_loop(0, half_m // 64, zero_tile, 0)

        pl.when(jnp.logical_and(t >= 1, t < steps + 1))(lambda: first_hop(t - 1))
        pl.when(jnp.logical_and(t >= 2, t < steps + 2))(lambda: second_hop(t - 2))
        pl.when(jnp.logical_and(t >= 3, t < steps + 3))(lambda: last_hop(t - 3))
        pl.when(jnp.logical_and(t >= LAG, t < steps + LAG - 1))(lambda: compute(t - LAG))
        return 0

    lax.fori_loop(0, steps + LAG, body, 0)

    q_last = steps - 1
    wait_inputs(q_last)
    quarter = half_m // 2
    chunk = quarter // 3

    def finish(row0):
        def tile(j, _):
            rows = pl.ds(al(row0), chunk)
            cols = pl.ds(al(j * tile_n), tile_n)
            total = acc[rows, cols] + jnp.dot(
                a_buf[q_last, rows, :], b_buf[q_last, :, cols], preferred_element_type=jnp.float32
            )
            c_st[rows, cols] = total.astype(c_st.dtype)
            return 0

        lax.fori_loop(0, 3, tile, 0)

    col_out = pl.ds(al(n * half_n), half_n)

    def c_remote(k):
        row0 = al((1 - e) * quarter + k * chunk)
        return pltpu.make_async_remote_copy(
            src_ref=c_st.at[pl.ds(row0, chunk), :],
            dst_ref=c_ref.at[pl.ds(al(k * chunk), chunk), col_out],
            send_sem=c_snd.at[k],
            recv_sem=c_rcv.at[k],
            device_id=dev_za,
            device_id_type=MESH,
        )

    def c_local(k):
        row0 = al(e * quarter + k * chunk)
        return pltpu.make_async_copy(c_st.at[pl.ds(row0, chunk), :], c_ref.at[pl.ds(al(k * chunk), chunk), col_out], c_loc.at[k])

    def out_partner(k, _):
        finish((1 - e) * quarter + k * chunk)
        c_remote(k).start()
        return 0

    def out_own(k, _):
        finish(e * quarter + k * chunk)
        c_local(k).start()
        return 0

    lax.fori_loop(0, 3, out_partner, 0)
    lax.fori_loop(0, 3, out_own, 0)

    def drain(q, _):
        for cp in a_own(q) + a_fwd(q) + b_own(q) + b_fwd(q):
            cp.wait_send()
        for which in range(3):
            a_z(q, which).wait_send()
            b_z(q, which).wait_send()
        for which in range(4):
            b_d2d(q, which).wait_send()
        return 0

    lax.fori_loop(0, steps, drain, 0)

    def drain_c(k, _):
        c_local(k).wait()
        c_remote(k).wait()
        return 0

    lax.fori_loop(0, 3, drain_c, 0)


def solution(mesh):
    assert (mesh.shape["depth"], mesh.shape["col"], mesh.shape["row"]) == (4, 4, 8)

    def local_mm(a_blk, b_blk):
        band, kblk = a_blk.shape
        seg = 128
        steps = band // seg
        half_m, half_n = band // 2, kblk // 2
        return pl.pallas_call(
            functools.partial(kernel, steps, seg),
            out_shape=jax.ShapeDtypeStruct((band // 4, kblk), jnp.bfloat16),
            in_specs=[pl.BlockSpec(memory_space=pl.ANY)] * 2,
            out_specs=pl.BlockSpec(memory_space=pl.ANY),
            scratch_shapes=[
                pltpu.VMEM((steps, half_m, 8 * seg), jnp.bfloat16),
                pltpu.VMEM((steps, 8 * seg, half_n), jnp.bfloat16),
                pltpu.VMEM((half_m, half_n), jnp.float32),
                pltpu.VMEM((half_m, half_n), jnp.bfloat16),
                pltpu.SemaphoreType.DMA((KINDS, steps)),
                pltpu.SemaphoreType.DMA((KINDS, steps)),
                pltpu.SemaphoreType.DMA((3, steps)),
                pltpu.SemaphoreType.DMA((3,)),
                pltpu.SemaphoreType.DMA((3,)),
                pltpu.SemaphoreType.DMA((3,)),
            ],
            compiler_params=pltpu.CompilerParams(collective_id=0, has_side_effects=True, vmem_limit_bytes=67043328),
            cost_estimate=pl.CostEstimate(
                flops=2 * half_m * half_n * 8 * band, bytes_accessed=4 * band * kblk, transcendentals=0
            ),
            name="gather_mm",
        )(a_blk, b_blk)

    spec_in = P("row", "col")
    spec_out = P(("row", "depth"), "col")
    return jax.shard_map(local_mm, mesh=mesh, in_specs=(spec_in, spec_in), out_specs=spec_out, check_vma=False)
```

```python
import functools

import jax
import jax.numpy as jnp
from jax import lax
from jax.experimental import pallas as pl
from jax.experimental.pallas import tpu as pltpu
from jax.sharding import PartitionSpec as P

MESH = pl.DeviceIdType.MESH

A_OWN, A_FWD, A_Z, B_OWN, B_FWD, B_Z, B_D2D, B_Z2, A_LOC, B_LOC = range(10)
KINDS = 10
SLOTS = 8

PHASES = ((192, 64, 768), (128, 32, 512), (64, 16, 256))
SEG = 256
EXCL_B = 80
AHEAD, HOP1, HOP2, HOP3, LAG = 0, 1, 2, 3, 4


def kernel(steps, a_ref, b_ref, c_ref, a_buf, b_buf, acc, c_st, snd, rcv, c_snd, c_rcv, c_loc):
    _, sub, kblk = a_ref.shape
    band, half_n = b_ref.shape[0], kblk // 2
    l = lax.axis_index("depth")
    y = lax.axis_index("col")
    i = lax.axis_index("row")
    x, c = i // 2, lax.rem(i, 2)
    h, e = l // 2, lax.rem(l, 2)
    n = lax.rem((l + 1) // 2, 2)
    role_a, role_b = e, h
    yp, ym, y2 = lax.rem(y + 1, 4), lax.rem(y + 3, 4), lax.rem(y + 2, 4)
    xp, xm, x2 = lax.rem(x + 1, 4), lax.rem(x + 3, 4), lax.rem(x + 2, 4)
    dev_yp, dev_ym = {"col": yp}, {"col": ym}
    dev_xp, dev_xm = {"row": 2 * xp + c}, {"row": 2 * xm + c}
    dev_za, dev_zb = {"depth": l + 1 - 2 * e}, {"depth": 3 - l}
    dev_sib = {"row": i + 1 - 2 * c}
    starts, r_at, c_at = [], 0, 0
    for rows, _, cols in PHASES:
        starts.append((r_at, c_at))
        r_at, c_at = r_at + rows, c_at + cols

    def al(v, m=128):
        return pl.multiple_of(v, m)

    def slot(ph, q):
        return lax.rem(ph * steps + q, SLOTS)

    def remote(kind, ph, q, src, dst, dev):
        return pltpu.make_async_remote_copy(
            src_ref=src,
            dst_ref=dst,
            send_sem=snd.at[B_Z if kind == B_Z2 else kind],
            recv_sem=rcv.at[kind, slot(ph, q)],
            device_id=dev,
            device_id_type=MESH,
        )

    def arrived(kind, ph, q):
        r0, (rows, excl, _) = starts[ph][0], PHASES[ph]
        if kind in (A_OWN, A_FWD, A_Z, A_LOC):
            count, width = {A_OWN: (rows - excl, 4), A_FWD: (rows - excl, 2), A_Z: (excl, 6), A_LOC: (rows, 2)}[kind]
            ref = a_buf.at[q, :, pl.ds(0, count), pl.ds(0, width * SEG)]
        else:
            carry = SEG - EXCL_B
            count = {B_OWN: 2 * carry, B_FWD: carry, B_Z: 2 * EXCL_B, B_Z2: EXCL_B, B_D2D: 4 * SEG, B_LOC: SEG}[kind]
            ref = b_buf.at[q, pl.ds(0, count), cols_b(ph)]
        pltpu.make_async_copy(ref, ref, rcv.at[kind, slot(ph, q)]).wait()

    def lanes_a(blk, p=0, width=2 * SEG):
        return pl.ds(al((2 * blk + p) * SEG), width)

    def a_own(ph, q):
        rows, excl, _ = PHASES[ph]
        carry = pl.ds(al(starts[ph][0] + excl * role_a, 16), rows - excl)
        out = []
        for d, dev in enumerate((dev_yp, dev_ym)):
            for p in range(2):
                src = a_ref.at[pl.ds(2 * h, 2), carry, pl.ds(al(p * band + q * SEG), SEG)]
                dst = a_buf.at[q, :, carry, lanes_a(y, p, SEG)]
                out.append(remote(A_OWN, ph, q, src, dst, dev))
        return out

    def a_fwd(ph, q):
        rows, excl, _ = PHASES[ph]
        carry = pl.ds(al(starts[ph][0] + excl * role_a, 16), rows - excl)
        out = []
        for d, (blk, dev) in enumerate(((ym, dev_yp), (yp, dev_ym))):
            ref = a_buf.at[q, :, carry, lanes_a(blk, d, SEG)]
            out.append(remote(A_FWD, ph, q, ref, ref, dev))
        return out

    def a_z(ph, q, which):
        rows, excl, _ = PHASES[ph]
        only = pl.ds(al(starts[ph][0] + (rows - excl) * role_a, 16), excl)
        ref = a_buf.at[q, :, only, lanes_a((ym, yp, y2)[which])]
        return remote(A_Z, ph, q, ref, ref, dev_za)

    def cols_b(ph, base=0):
        return pl.ds(al(base + starts[ph][1]), PHASES[ph][2])

    def b_own(ph, q):
        out = []
        for d, dev in enumerate((dev_xp, dev_xm)):
            src = b_ref.at[pl.ds(al(q * SEG + EXCL_B * role_b, 16), SEG - EXCL_B), cols_b(ph, n * half_n)]
            dst = b_buf.at[q, pl.ds(al((2 * x + c) * SEG + EXCL_B * role_b, 16), SEG - EXCL_B), cols_b(ph)]
            out.append(remote(B_OWN, ph, q, src, dst, dev))
        return out

    def b_fwd(ph, q):
        half = PHASES[ph][2] // 2
        out = []
        for d, (blk, dev) in enumerate(((xm, dev_xp), (xp, dev_xm))):
            ref = b_buf.at[
                q,
                pl.ds(al((2 * blk + c) * SEG + EXCL_B * role_b, 16), SEG - EXCL_B),
                pl.ds(starts[ph][1] + d * half, half),
            ]
            out.append(remote(B_FWD, ph, q, ref, ref, dev))
        return out

    def b_z(ph, q, which):
        blk = (xm, xp, x2)[which]
        ref = b_buf.at[q, pl.ds(al((2 * blk + c) * SEG + (SEG - EXCL_B) * role_b, 16), EXCL_B), cols_b(ph)]
        return remote(B_Z2 if which == 2 else B_Z, ph, q, ref, ref, dev_zb)

    def b_d2d(ph, q, which):
        blk = (xm, xp, x2, x)[which]
        dst = b_buf.at[q, pl.ds(al((2 * blk + c) * SEG), SEG), cols_b(ph)]
        src = b_ref.at[pl.ds(al(q * SEG), SEG), cols_b(ph, n * half_n)] if which == 3 else dst
        return remote(B_D2D, ph, q, src, dst, dev_sib)

    def local(ph, q):
        rows = pl.ds(starts[ph][0], PHASES[ph][0])
        out = []
        for p in range(2):
            src = a_ref.at[pl.ds(2 * h, 2), rows, pl.ds(al(p * band + q * SEG), SEG)]
            dst = a_buf.at[q, :, rows, lanes_a(y, p, SEG)]
            out.append(pltpu.make_async_copy(src, dst, rcv.at[A_LOC, slot(ph, q)]))
        src = b_ref.at[pl.ds(al(q * SEG), SEG), cols_b(ph, n * half_n)]
        dst = b_buf.at[q, pl.ds(al((2 * x + c) * SEG), SEG), cols_b(ph)]
        out.append(pltpu.make_async_copy(src, dst, rcv.at[B_LOC, slot(ph, q)]))
        return out

    barrier = pltpu.get_barrier_semaphore()
    partners = (dev_yp, dev_ym, dev_xp, dev_xm, dev_za, dev_zb, dev_sib)
    for dev in partners:
        pl.semaphore_signal(barrier, inc=1, device_id=dev, device_id_type=MESH)
    pl.semaphore_wait(barrier, len(partners))

    def send_own(ph, q):
        for cp in b_own(ph, q) + a_own(ph, q) + [b_d2d(ph, q, 3)] + local(ph, q):
            cp.start()

    def first_hop(ph, q):
        arrived(B_OWN, ph, q)
        for cp in b_fwd(ph, q) + [b_z(ph, q, 0), b_z(ph, q, 1)]:
            cp.start()
        arrived(A_OWN, ph, q)
        for cp in a_fwd(ph, q) + [a_z(ph, q, 0), a_z(ph, q, 1)]:
            cp.start()

    def second_hop(ph, q):
        arrived(B_FWD, ph, q)
        b_z(ph, q, 2).start()
        arrived(A_FWD, ph, q)
        a_z(ph, q, 2).start()
        arrived(B_Z, ph, q)
        for which in range(2):
            b_d2d(ph, q, which).start()

    def last_hop(ph, q):
        arrived(B_Z2, ph, q)
        b_d2d(ph, q, 2).start()

    def mm(q, r0, rows, col, width):
        a_val = a_buf[q, :, r0 : r0 + rows, :].reshape(2 * rows, 8 * SEG)
        prod = jnp.dot(a_val, b_buf[q, :, pl.ds(col, width)], preferred_element_type=jnp.float32)
        at = (slice(None), slice(r0, r0 + rows), pl.ds(col, width))
        old = jnp.where(q == 0, 0.0, acc[at])
        acc[at] = old + prod.reshape(2, rows, width)

    def strips(ph):
        (r0, c0), (rows, _, cols) = starts[ph], PHASES[ph]
        return ([(0, r0, c0, cols)] if r0 else []) + [(r0, rows, 0, c0 + cols)]

    col_base = n * half_n

    def c_copy(ph, k):
        r0, rows, c0, cols = strips(ph)[k]
        dst = c_ref.at[pl.ds(r0, rows), pl.ds(al(col_base + c0), cols)]
        part = (pl.ds(r0, rows), pl.ds(c0, cols))
        idx = 2 * ph + k
        out = pltpu.make_async_remote_copy(
            src_ref=c_st.at[(1 - e, *part)],
            dst_ref=dst,
            send_sem=c_snd.at[idx],
            recv_sem=c_rcv.at[idx],
            device_id=dev_za,
            device_id_type=MESH,
        )
        return out, pltpu.make_async_copy(c_st.at[(e, *part)], dst, c_loc.at[idx])

    def compute(ph, q):
        for kind in (A_LOC, B_LOC, A_Z, B_D2D):
            arrived(kind, ph, q)
        for k, (r0, rows, c0, cols) in enumerate(strips(ph)):
            mm(q, r0, rows, c0, cols)

            @pl.when(q == steps - 1)
            def _(k=k, r0=r0, rows=rows, c0=c0, cols=cols):
                tile = 256

                def round_tile(j, _, tile=tile):
                    at = (slice(None), slice(r0, r0 + rows), pl.ds(al(c0 + j * tile), tile))
                    c_st[at] = acc[at].astype(c_st.dtype)
                    return 0

                lax.fori_loop(0, cols // tile, round_tile, 0)
                for cp in c_copy(ph, k):
                    cp.start()

    total = len(PHASES) * steps

    def stage(t, delay, fn):
        for ph in range(len(PHASES)):
            q = t - delay - ph * steps
            pl.when(jnp.logical_and(q >= 0, q < steps))(lambda ph=ph, q=q: fn(ph, q))

    for s in range(AHEAD):
        send_own(s // steps, s % steps)

    def body(t, _):
        stage(t, -AHEAD, send_own)
        stage(t, HOP1, first_hop)
        stage(t, HOP2, second_hop)
        stage(t, HOP3, last_hop)
        stage(t, LAG, compute)
        return 0

    lax.fori_loop(0, total + LAG, body, 0)

    carry_a, excl_a = sum(p[0] - p[1] for p in PHASES), sum(p[1] for p in PHASES)
    sent_a = {A_OWN: (carry_a, 4), A_FWD: (carry_a, 2), A_Z: (excl_a, 6)}
    sent_b = {B_OWN: 2 * (SEG - EXCL_B), B_FWD: SEG - EXCL_B, B_Z: 3 * EXCL_B, B_D2D: 4 * SEG}
    for kind, (count, width) in sent_a.items():
        ref = a_buf.at[:, :, pl.ds(0, count), pl.ds(0, width * SEG)]
        pltpu.make_async_copy(ref, ref, snd.at[kind]).wait()
    for kind, count in sent_b.items():
        ref = b_buf.at[:, pl.ds(0, count), :]
        pltpu.make_async_copy(ref, ref, snd.at[kind]).wait()
    for ph in range(len(PHASES)):
        for k in range(len(strips(ph))):
            for cp in c_copy(ph, k):
                cp.wait()


def solution(mesh):
    assert (mesh.shape["depth"], mesh.shape["col"], mesh.shape["row"]) == (4, 4, 8)

    def local_mm(a_blk, b_blk):
        band, kblk = a_blk.shape
        sub, half_n, steps = band // 4, kblk // 2, band // SEG
        assert sum(p[0] for p in PHASES) == sub and sum(p[2] for p in PHASES) == half_n
        return pl.pallas_call(
            functools.partial(kernel, steps),
            out_shape=jax.ShapeDtypeStruct((sub, kblk), jnp.bfloat16),
            in_specs=[pl.BlockSpec(memory_space=pl.ANY)] * 2,
            out_specs=pl.BlockSpec(memory_space=pl.ANY),
            scratch_shapes=[
                pltpu.VMEM((steps, 2, sub, 8 * SEG), jnp.bfloat16),
                pltpu.VMEM((steps, 8 * SEG, half_n), jnp.bfloat16),
                pltpu.VMEM((2, sub, half_n), jnp.float32),
                pltpu.VMEM((2, sub, half_n), jnp.bfloat16),
                pltpu.SemaphoreType.DMA((B_Z2,)),
                pltpu.SemaphoreType.DMA((KINDS, SLOTS)),
                pltpu.SemaphoreType.DMA((2 * len(PHASES),)),
                pltpu.SemaphoreType.DMA((2 * len(PHASES),)),
                pltpu.SemaphoreType.DMA((2 * len(PHASES),)),
            ],
            compiler_params=pltpu.CompilerParams(collective_id=0, has_side_effects=True, vmem_limit_bytes=67043328),
            cost_estimate=pl.CostEstimate(
                flops=4 * sub * half_n * 8 * band, bytes_accessed=4 * band * kblk, transcendentals=0
            ),
            name="gather_mm",
        )(a_blk.reshape(4, sub, kblk), b_blk)

    spec_in = P("row", "col")
    spec_out = P(("row", "depth"), "col")
    return jax.shard_map(local_mm, mesh=mesh, in_specs=(spec_in, spec_in), out_specs=spec_out, check_vma=False)
```

```python
import functools

import jax
import jax.numpy as jnp
from jax import lax
from jax.experimental import pallas as pl
from jax.experimental.pallas import tpu as pltpu
from jax.sharding import PartitionSpec as P

MESH = pl.DeviceIdType.MESH

A_OWN, A_FWD, A_Z, B_OWN, B_FWD, B_Z, B_D2D, B_Z2, A_LOC, B_LOC = range(10)
KINDS = 10
SLOTS = 8

PHASES = ((192, 64, 768), (128, 32, 512), (64, 16, 256))
WIDTHS = ((768,), (512, 640), (256, 768))
SEG = 256
EXCL_B = 80
HOP1, HOP2, HOP3, LAG = 1, 2, 3, 4
LATE = ((1, 1),)


def kernel(steps, a_ref, b_ref, c_ref, a_buf, b_buf, acc, c_st, snd, rcv, c_snd, c_rcv, c_loc):
    _, sub, kblk = a_ref.shape
    band, half_n = b_ref.shape[0], kblk // 2
    l = lax.axis_index("depth")
    y = lax.axis_index("col")
    i = lax.axis_index("row")
    x, c = i // 2, lax.rem(i, 2)
    h, e = l // 2, lax.rem(l, 2)
    n = lax.rem((l + 1) // 2, 2)
    role_a, role_b = e, h
    yp, ym, y2 = lax.rem(y + 1, 4), lax.rem(y + 3, 4), lax.rem(y + 2, 4)
    xp, xm, x2 = lax.rem(x + 1, 4), lax.rem(x + 3, 4), lax.rem(x + 2, 4)
    dev_yp, dev_ym = {"col": yp}, {"col": ym}
    dev_xp, dev_xm = {"row": 2 * xp + c}, {"row": 2 * xm + c}
    dev_za, dev_zb = {"depth": l + 1 - 2 * e}, {"depth": 3 - l}
    dev_sib = {"row": i + 1 - 2 * c}
    starts, r_at, c_at = [], 0, 0
    for rows, _, cols in PHASES:
        starts.append((r_at, c_at))
        r_at, c_at = r_at + rows, c_at + cols

    def al(v, m=128):
        return pl.multiple_of(v, m)

    def slot(ph, q):
        return lax.rem(ph * steps + q, SLOTS)

    def remote(kind, ph, q, src, dst, dev):
        return pltpu.make_async_remote_copy(
            src_ref=src,
            dst_ref=dst,
            send_sem=snd.at[B_Z if kind == B_Z2 else kind],
            recv_sem=rcv.at[kind, slot(ph, q)],
            device_id=dev,
            device_id_type=MESH,
        )

    def arrived(kind, ph, q):
        r0, (rows, excl, _) = starts[ph][0], PHASES[ph]
        if kind in (A_OWN, A_FWD, A_Z, A_LOC):
            count, width = {A_OWN: (rows - excl, 4), A_FWD: (rows - excl, 2), A_Z: (excl, 6), A_LOC: (rows, 2)}[kind]
            ref = a_buf.at[q, :, pl.ds(0, count), pl.ds(0, width * SEG)]
        else:
            carry = SEG - EXCL_B
            count = {B_OWN: 2 * carry, B_FWD: carry, B_Z: 2 * EXCL_B, B_Z2: EXCL_B, B_D2D: 4 * SEG, B_LOC: SEG}[kind]
            ref = b_buf.at[q, pl.ds(0, count), cols_b(ph)]
        pltpu.make_async_copy(ref, ref, rcv.at[kind, slot(ph, q)]).wait()

    def lanes_a(blk, p=0, width=2 * SEG):
        return pl.ds(al((2 * blk + p) * SEG), width)

    def a_own(ph, q):
        rows, excl, _ = PHASES[ph]
        carry = pl.ds(al(starts[ph][0] + excl * role_a, 8), rows - excl)
        out = []
        for d, dev in enumerate((dev_yp, dev_ym)):
            for p in range(2):
                src = a_ref.at[pl.ds(2 * h, 2), carry, pl.ds(al(p * band + q * SEG), SEG)]
                dst = a_buf.at[q, :, carry, lanes_a(y, p, SEG)]
                out.append(remote(A_OWN, ph, q, src, dst, dev))
        return out

    def a_fwd(ph, q):
        rows, excl, _ = PHASES[ph]
        carry = pl.ds(al(starts[ph][0] + excl * role_a, 8), rows - excl)
        out = []
        for d, (blk, dev) in enumerate(((ym, dev_yp), (yp, dev_ym))):
            ref = a_buf.at[q, :, carry, lanes_a(blk, d, SEG)]
            out.append(remote(A_FWD, ph, q, ref, ref, dev))
        return out

    def a_z(ph, q, which):
        rows, excl, _ = PHASES[ph]
        only = pl.ds(al(starts[ph][0] + (rows - excl) * role_a, 8), excl)
        ref = a_buf.at[q, :, only, lanes_a((ym, yp, y2)[which])]
        return remote(A_Z, ph, q, ref, ref, dev_za)

    def cols_b(ph, base=0):
        return pl.ds(al(base + starts[ph][1]), PHASES[ph][2])

    def b_own(ph, q):
        out = []
        for d, dev in enumerate((dev_xp, dev_xm)):
            src = b_ref.at[pl.ds(al(q * SEG + EXCL_B * role_b, 16), SEG - EXCL_B), cols_b(ph, n * half_n)]
            dst = b_buf.at[q, pl.ds(al((2 * x + c) * SEG + EXCL_B * role_b, 16), SEG - EXCL_B), cols_b(ph)]
            out.append(remote(B_OWN, ph, q, src, dst, dev))
        return out

    def b_fwd(ph, q):
        half = PHASES[ph][2] // 2
        out = []
        for d, (blk, dev) in enumerate(((xm, dev_xp), (xp, dev_xm))):
            ref = b_buf.at[
                q,
                pl.ds(al((2 * blk + c) * SEG + EXCL_B * role_b, 16), SEG - EXCL_B),
                pl.ds(starts[ph][1] + d * half, half),
            ]
            out.append(remote(B_FWD, ph, q, ref, ref, dev))
        return out

    def b_z(ph, q, which):
        blk = (xm, xp, x2)[which]
        ref = b_buf.at[q, pl.ds(al((2 * blk + c) * SEG + (SEG - EXCL_B) * role_b, 16), EXCL_B), cols_b(ph)]
        return remote(B_Z2 if which == 2 else B_Z, ph, q, ref, ref, dev_zb)

    def b_d2d(ph, q, which):
        blk = (xm, xp, x2, x)[which]
        dst = b_buf.at[q, pl.ds(al((2 * blk + c) * SEG), SEG), cols_b(ph)]
        src = b_ref.at[pl.ds(al(q * SEG), SEG), cols_b(ph, n * half_n)] if which == 3 else dst
        return remote(B_D2D, ph, q, src, dst, dev_sib)

    def local(ph, q):
        rows = pl.ds(starts[ph][0], PHASES[ph][0])
        out = []
        for p in range(2):
            src = a_ref.at[pl.ds(2 * h, 2), rows, pl.ds(al(p * band + q * SEG), SEG)]
            dst = a_buf.at[q, :, rows, lanes_a(y, p, SEG)]
            out.append(pltpu.make_async_copy(src, dst, rcv.at[A_LOC, slot(ph, q)]))
        src = b_ref.at[pl.ds(al(q * SEG), SEG), cols_b(ph, n * half_n)]
        dst = b_buf.at[q, pl.ds(al((2 * x + c) * SEG), SEG), cols_b(ph)]
        out.append(pltpu.make_async_copy(src, dst, rcv.at[B_LOC, slot(ph, q)]))
        return out

    barrier = pltpu.get_barrier_semaphore()
    partners = (dev_yp, dev_ym, dev_xp, dev_xm, dev_za, dev_zb, dev_sib)
    for dev in partners:
        pl.semaphore_signal(barrier, inc=1, device_id=dev, device_id_type=MESH)
    pl.semaphore_wait(barrier, len(partners))

    def send_own(ph, q):
        for cp in b_own(ph, q) + a_own(ph, q) + [b_d2d(ph, q, 3)] + local(ph, q):
            cp.start()

    def first_hop(ph, q):
        arrived(B_OWN, ph, q)
        for cp in b_fwd(ph, q) + [b_z(ph, q, 0), b_z(ph, q, 1)]:
            cp.start()
        arrived(A_OWN, ph, q)
        for cp in a_fwd(ph, q) + [a_z(ph, q, 0), a_z(ph, q, 1)]:
            cp.start()

    def second_hop(ph, q):
        arrived(B_FWD, ph, q)
        b_z(ph, q, 2).start()
        arrived(A_FWD, ph, q)
        a_z(ph, q, 2).start()
        arrived(B_Z, ph, q)
        for which in range(2):
            b_d2d(ph, q, which).start()

    def last_hop(ph, q):
        arrived(B_Z2, ph, q)
        b_d2d(ph, q, 2).start()

    def mm(q, r0, rows, col, width):
        a_val = a_buf[q, :, r0 : r0 + rows, :].reshape(2 * rows, 8 * SEG)
        prod = jnp.dot(a_val, b_buf[q, :, pl.ds(col, width)], preferred_element_type=jnp.float32)
        at = (slice(None), slice(r0, r0 + rows), pl.ds(col, width))
        old = jnp.where(q == 0, 0.0, acc[at])
        acc[at] = old + prod.reshape(2, rows, width)

    def strips(ph):
        (r0, c0), (rows, _, cols) = starts[ph], PHASES[ph]
        return ([(0, r0, c0, cols)] if r0 else []) + [(r0, rows, 0, c0 + cols)]

    col_base = n * half_n

    def c_copy(ph, k):
        r0, rows, c0, cols = strips(ph)[k]
        dst = c_ref.at[pl.ds(r0, rows), pl.ds(al(col_base + c0), cols)]
        part = (pl.ds(r0, rows), pl.ds(c0, cols))
        idx = 2 * ph + k
        out = pltpu.make_async_remote_copy(
            src_ref=c_st.at[(1 - e, *part)],
            dst_ref=dst,
            send_sem=c_snd.at[idx],
            recv_sem=c_rcv.at[idx],
            device_id=dev_za,
            device_id_type=MESH,
        )
        return out, pltpu.make_async_copy(c_st.at[(e, *part)], dst, c_loc.at[idx])

    def compute(ph, q):
        for kind in (A_LOC, B_LOC, A_Z, B_D2D):
            arrived(kind, ph, q)
        for k, (r0, rows, c0, cols) in enumerate(strips(ph)):
            wide = WIDTHS[ph][k]

            def col_tile(j, _, r0=r0, rows=rows, c0=c0, wide=wide):
                mm(q, r0, rows, al(c0 + j * wide), wide)
                return 0

            lax.fori_loop(0, cols // wide, col_tile, 0)

            @pl.when(q == steps - 1)
            def _(k=k, r0=r0, rows=rows, c0=c0, cols=cols):
                tile = 256

                def round_tile(j, _, tile=tile):
                    at = (slice(None), slice(r0, r0 + rows), pl.ds(al(c0 + j * tile), tile))
                    c_st[at] = acc[at].astype(c_st.dtype)
                    return 0

                lax.fori_loop(0, cols // tile, round_tile, 0)
                if (ph, k) not in LATE:
                    for cp in c_copy(ph, k):
                        cp.start()

    total = len(PHASES) * steps

    def stage(t, delay, fn):
        for ph in range(len(PHASES)):
            q = t - delay - ph * steps
            pl.when(jnp.logical_and(q >= 0, q < steps))(lambda ph=ph, q=q: fn(ph, q))

    def body(t, _):
        stage(t, 0, send_own)
        stage(t, HOP1, first_hop)
        stage(t, HOP2, second_hop)
        if LATE:

            @pl.when(t == total - 1 + HOP2)
            def _():
                for ph, k in LATE:
                    for cp in c_copy(ph, k):
                        cp.start()

        stage(t, HOP3, last_hop)
        stage(t, LAG, compute)
        return 0

    lax.fori_loop(0, total + LAG, body, 0)

    carry_a, excl_a = sum(p[0] - p[1] for p in PHASES), sum(p[1] for p in PHASES)
    sent_a = {A_OWN: (carry_a, 4), A_FWD: (carry_a, 2), A_Z: (excl_a, 6)}
    sent_b = {B_OWN: 2 * (SEG - EXCL_B), B_FWD: SEG - EXCL_B, B_Z: 3 * EXCL_B, B_D2D: 4 * SEG}
    for kind, (count, width) in sent_a.items():
        ref = a_buf.at[:, :, pl.ds(0, count), pl.ds(0, width * SEG)]
        pltpu.make_async_copy(ref, ref, snd.at[kind]).wait()
    for kind, count in sent_b.items():
        ref = b_buf.at[:, pl.ds(0, count), :]
        pltpu.make_async_copy(ref, ref, snd.at[kind]).wait()
    for ph in range(len(PHASES)):
        for k in range(len(strips(ph))):
            for cp in c_copy(ph, k):
                cp.wait()


def solution(mesh):
    assert (mesh.shape["depth"], mesh.shape["col"], mesh.shape["row"]) == (4, 4, 8)

    def local_mm(a_blk, b_blk):
        band, kblk = a_blk.shape
        sub, half_n, steps = band // 4, kblk // 2, band // SEG
        assert sum(p[0] for p in PHASES) == sub and sum(p[2] for p in PHASES) == half_n
        return pl.pallas_call(
            functools.partial(kernel, steps),
            out_shape=jax.ShapeDtypeStruct((sub, kblk), jnp.bfloat16),
            in_specs=[pl.BlockSpec(memory_space=pl.ANY)] * 2,
            out_specs=pl.BlockSpec(memory_space=pl.ANY),
            scratch_shapes=[
                pltpu.VMEM((steps, 2, sub, 8 * SEG), jnp.bfloat16),
                pltpu.VMEM((steps, 8 * SEG, half_n), jnp.bfloat16),
                pltpu.VMEM((2, sub, half_n), jnp.float32),
                pltpu.VMEM((2, sub, half_n), jnp.bfloat16),
                pltpu.SemaphoreType.DMA((B_Z2,)),
                pltpu.SemaphoreType.DMA((KINDS, SLOTS)),
                pltpu.SemaphoreType.DMA((2 * len(PHASES),)),
                pltpu.SemaphoreType.DMA((2 * len(PHASES),)),
                pltpu.SemaphoreType.DMA((2 * len(PHASES),)),
            ],
            compiler_params=pltpu.CompilerParams(collective_id=0, has_side_effects=True, vmem_limit_bytes=67043328),
            cost_estimate=pl.CostEstimate(
                flops=4 * sub * half_n * 8 * band, bytes_accessed=4 * band * kblk, transcendentals=0
            ),
            name="gather_mm",
        )(a_blk.reshape(4, sub, kblk), b_blk)

    spec_in = P("row", "col")
    spec_out = P(("row", "depth"), "col")
    return jax.shard_map(local_mm, mesh=mesh, in_specs=(spec_in, spec_in), out_specs=spec_out, check_vma=False)
```

```python
import functools

import jax
import jax.numpy as jnp
from jax import lax
from jax.experimental import pallas as pl
from jax.experimental.pallas import tpu as pltpu
from jax.sharding import PartitionSpec as P

MESH = pl.DeviceIdType.MESH

A_OWN, A_FWD, A_Z, B_OWN, B_FWD, B_Z, B_D2D, B_Z2, A_LOC, B_LOC = range(10)
KINDS = 10
SLOTS = 8

PHASES = ((192, 64, 768), (128, 32, 512), (64, 16, 256))
WIDTHS = ((768,), (512, 640), (256, 768))
SEG = 256
EXCL_B = 80
HOP1, HOP2, HOP3, LAG = 1, 2, 3, 4
LATE = ((1, 1),)


def kernel(steps, a_ref, b_ref, c_ref, a_buf, b_buf, acc, c_st, snd, rcv, c_snd, c_rcv, c_loc):
    _, sub, kblk = a_ref.shape
    band, half_n = b_ref.shape[0], kblk // 2
    l = lax.axis_index("depth")
    y = lax.axis_index("col")
    i = lax.axis_index("row")
    x, c = i // 2, lax.rem(i, 2)
    h, e = l // 2, lax.rem(l, 2)
    n = lax.rem((l + 1) // 2, 2)
    role_a, role_b = e, h
    yp, ym, y2 = lax.rem(y + 1, 4), lax.rem(y + 3, 4), lax.rem(y + 2, 4)
    xp, xm, x2 = lax.rem(x + 1, 4), lax.rem(x + 3, 4), lax.rem(x + 2, 4)
    dev_yp, dev_ym = {"col": yp}, {"col": ym}
    dev_xp, dev_xm = {"row": 2 * xp + c}, {"row": 2 * xm + c}
    dev_za, dev_zb = {"depth": l + 1 - 2 * e}, {"depth": 3 - l}
    dev_sib = {"row": i + 1 - 2 * c}
    starts, r_at, c_at = [], 0, 0
    for rows, _, cols in PHASES:
        starts.append((r_at, c_at))
        r_at, c_at = r_at + rows, c_at + cols

    def al(v, m=128):
        return pl.multiple_of(v, m)

    def slot(ph, q):
        return lax.rem(ph * steps + q, SLOTS)

    def remote(kind, ph, q, src, dst, dev):
        return pltpu.make_async_remote_copy(
            src_ref=src,
            dst_ref=dst,
            send_sem=snd.at[B_Z if kind == B_Z2 else kind],
            recv_sem=rcv.at[kind, slot(ph, q)],
            device_id=dev,
            device_id_type=MESH,
        )

    def arrived(kind, ph, q):
        r0, (rows, excl, _) = starts[ph][0], PHASES[ph]
        if kind in (A_OWN, A_FWD, A_Z, A_LOC):
            count, width = {A_OWN: (rows - excl, 4), A_FWD: (rows - excl, 2), A_Z: (excl, 6), A_LOC: (rows, 2)}[kind]
            ref = a_buf.at[q, :, pl.ds(0, count), pl.ds(0, width * SEG)]
        else:
            carry = SEG - EXCL_B
            count = {B_OWN: 2 * carry, B_FWD: carry, B_Z: 2 * EXCL_B, B_Z2: EXCL_B, B_D2D: 4 * SEG, B_LOC: SEG}[kind]
            ref = b_buf.at[q, pl.ds(0, count), cols_b(ph)]
        pltpu.make_async_copy(ref, ref, rcv.at[kind, slot(ph, q)]).wait()

    def lanes_a(blk, p=0, width=2 * SEG):
        return pl.ds(al((2 * blk + p) * SEG), width)

    def a_own(ph, q):
        rows, excl, _ = PHASES[ph]
        carry = pl.ds(al(starts[ph][0] + excl * role_a, 8), rows - excl)
        out = []
        for d, dev in enumerate((dev_yp, dev_ym)):
            for p in range(2):
                src = a_ref.at[pl.ds(2 * h, 2), carry, pl.ds(al(p * band + q * SEG), SEG)]
                dst = a_buf.at[q, :, carry, lanes_a(y, p, SEG)]
                out.append(remote(A_OWN, ph, q, src, dst, dev))
        return out

    def a_fwd(ph, q):
        rows, excl, _ = PHASES[ph]
        carry = pl.ds(al(starts[ph][0] + excl * role_a, 8), rows - excl)
        out = []
        for d, (blk, dev) in enumerate(((ym, dev_yp), (yp, dev_ym))):
            ref = a_buf.at[q, :, carry, lanes_a(blk, d, SEG)]
            out.append(remote(A_FWD, ph, q, ref, ref, dev))
        return out

    def a_z(ph, q, which):
        rows, excl, _ = PHASES[ph]
        only = pl.ds(al(starts[ph][0] + (rows - excl) * role_a, 8), excl)
        ref = a_buf.at[q, :, only, lanes_a((ym, yp, y2)[which])]
        return remote(A_Z, ph, q, ref, ref, dev_za)

    def cols_b(ph, base=0):
        return pl.ds(al(base + starts[ph][1]), PHASES[ph][2])

    def b_own(ph, q):
        out = []
        for d, dev in enumerate((dev_xp, dev_xm)):
            src = b_ref.at[pl.ds(al(q * SEG + EXCL_B * role_b, 16), SEG - EXCL_B), cols_b(ph, n * half_n)]
            dst = b_buf.at[q, pl.ds(al((2 * x + c) * SEG + EXCL_B * role_b, 16), SEG - EXCL_B), cols_b(ph)]
            out.append(remote(B_OWN, ph, q, src, dst, dev))
        return out

    def b_fwd(ph, q):
        half = PHASES[ph][2] // 2
        out = []
        for d, (blk, dev) in enumerate(((xm, dev_xp), (xp, dev_xm))):
            ref = b_buf.at[
                q,
                pl.ds(al((2 * blk + c) * SEG + EXCL_B * role_b, 16), SEG - EXCL_B),
                pl.ds(starts[ph][1] + d * half, half),
            ]
            out.append(remote(B_FWD, ph, q, ref, ref, dev))
        return out

    def b_z(ph, q, which):
        blk = (xm, xp, x2)[which]
        ref = b_buf.at[q, pl.ds(al((2 * blk + c) * SEG + (SEG - EXCL_B) * role_b, 16), EXCL_B), cols_b(ph)]
        return remote(B_Z2 if which == 2 else B_Z, ph, q, ref, ref, dev_zb)

    def b_d2d(ph, q, which):
        blk = (xm, xp, x2, x)[which]
        dst = b_buf.at[q, pl.ds(al((2 * blk + c) * SEG), SEG), cols_b(ph)]
        src = b_ref.at[pl.ds(al(q * SEG), SEG), cols_b(ph, n * half_n)] if which == 3 else dst
        return remote(B_D2D, ph, q, src, dst, dev_sib)

    def local(ph, q):
        rows = pl.ds(starts[ph][0], PHASES[ph][0])
        out = []
        for p in range(2):
            src = a_ref.at[pl.ds(2 * h, 2), rows, pl.ds(al(p * band + q * SEG), SEG)]
            dst = a_buf.at[q, :, rows, lanes_a(y, p, SEG)]
            out.append(pltpu.make_async_copy(src, dst, rcv.at[A_LOC, slot(ph, q)]))
        src = b_ref.at[pl.ds(al(q * SEG), SEG), cols_b(ph, n * half_n)]
        dst = b_buf.at[q, pl.ds(al((2 * x + c) * SEG), SEG), cols_b(ph)]
        out.append(pltpu.make_async_copy(src, dst, rcv.at[B_LOC, slot(ph, q)]))
        return out

    barrier = pltpu.get_barrier_semaphore()
    partners = (dev_yp, dev_ym, dev_xp, dev_xm, dev_za, dev_zb, dev_sib)
    for dev in partners:
        pl.semaphore_signal(barrier, inc=1, device_id=dev, device_id_type=MESH)
    pl.semaphore_wait(barrier, len(partners))

    def send_own(ph, q):
        for cp in b_own(ph, q) + a_own(ph, q) + [b_d2d(ph, q, 3)] + local(ph, q):
            cp.start()

    def first_hop(ph, q):
        arrived(B_OWN, ph, q)
        for cp in b_fwd(ph, q) + [b_z(ph, q, 0), b_z(ph, q, 1)]:
            cp.start()
        arrived(A_OWN, ph, q)
        for cp in a_fwd(ph, q) + [a_z(ph, q, 0), a_z(ph, q, 1)]:
            cp.start()

    def second_hop(ph, q):
        arrived(B_FWD, ph, q)
        b_z(ph, q, 2).start()
        arrived(A_FWD, ph, q)
        a_z(ph, q, 2).start()
        arrived(B_Z, ph, q)
        for which in range(2):
            b_d2d(ph, q, which).start()

    def last_hop(ph, q):
        arrived(B_Z2, ph, q)
        b_d2d(ph, q, 2).start()

    def mm(q, r0, rows, col, width):
        a_val = a_buf[q, :, r0 : r0 + rows, :].reshape(2 * rows, 8 * SEG)
        prod = jnp.dot(a_val, b_buf[q, :, pl.ds(col, width)], preferred_element_type=jnp.float32)
        at = (slice(None), slice(r0, r0 + rows), pl.ds(col, width))
        old = jnp.where(q == 0, 0.0, acc[at])
        acc[at] = old + prod.reshape(2, rows, width)

    def strips(ph):
        (r0, c0), (rows, _, cols) = starts[ph], PHASES[ph]
        return ([(0, r0, c0, cols)] if r0 else []) + [(r0, rows, 0, c0 + cols)]

    col_base = n * half_n

    def c_copy(ph, k):
        r0, rows, c0, cols = strips(ph)[k]
        dst = c_ref.at[pl.ds(r0, rows), pl.ds(al(col_base + c0), cols)]
        part = (pl.ds(r0, rows), pl.ds(c0, cols))
        out = pltpu.make_async_remote_copy(
            src_ref=c_st.at[(1 - e, *part)],
            dst_ref=dst,
            send_sem=c_snd,
            recv_sem=c_rcv,
            device_id=dev_za,
            device_id_type=MESH,
        )
        return out, pltpu.make_async_copy(c_st.at[(e, *part)], dst, c_loc)

    def compute(ph, q):
        for kind in (A_LOC, B_LOC, A_Z, B_D2D):
            arrived(kind, ph, q)
        for k, (r0, rows, c0, cols) in enumerate(strips(ph)):
            wide = WIDTHS[ph][k]

            def col_tile(j, _, r0=r0, rows=rows, c0=c0, wide=wide):
                mm(q, r0, rows, al(c0 + j * wide), wide)
                return 0

            lax.fori_loop(0, cols // wide, col_tile, 0)

            @pl.when(q == steps - 1)
            def _(k=k, r0=r0, rows=rows, c0=c0, cols=cols):
                tile = 256

                def round_tile(j, _, tile=tile):
                    at = (slice(None), slice(r0, r0 + rows), pl.ds(al(c0 + j * tile), tile))
                    c_st[at] = acc[at].astype(c_st.dtype)
                    return 0

                lax.fori_loop(0, cols // tile, round_tile, 0)
                if (ph, k) not in LATE:
                    for cp in c_copy(ph, k):
                        cp.start()

    total = len(PHASES) * steps

    def stage(t, delay, fn):
        for ph in range(len(PHASES)):
            q = t - delay - ph * steps
            pl.when(jnp.logical_and(q >= 0, q < steps))(lambda ph=ph, q=q: fn(ph, q))

    def body(t, _):
        stage(t, 0, send_own)
        stage(t, HOP1, first_hop)
        stage(t, HOP2, second_hop)
        if LATE:

            @pl.when(t == total - 1 + HOP2)
            def _():
                for ph, k in LATE:
                    for cp in c_copy(ph, k):
                        cp.start()

        stage(t, HOP3, last_hop)
        stage(t, LAG, compute)
        return 0

    lax.fori_loop(0, total + LAG, body, 0)

    carry_a, excl_a = sum(p[0] - p[1] for p in PHASES), sum(p[1] for p in PHASES)
    sent_a = {A_OWN: (carry_a, 4), A_FWD: (carry_a, 2), A_Z: (excl_a, 6)}
    sent_b = {B_OWN: 2 * (SEG - EXCL_B), B_FWD: SEG - EXCL_B, B_Z: 3 * EXCL_B, B_D2D: 4 * SEG}
    for kind, (count, width) in sent_a.items():
        ref = a_buf.at[:, :, pl.ds(0, count), pl.ds(0, width * SEG)]
        pltpu.make_async_copy(ref, ref, snd.at[kind]).wait()
    for kind, count in sent_b.items():
        ref = b_buf.at[:, pl.ds(0, count), :]
        pltpu.make_async_copy(ref, ref, snd.at[kind]).wait()
    for sem in (c_snd, c_rcv, c_loc):
        pltpu.make_async_copy(c_st.at[0], c_st.at[0], sem).wait()


def put_out(c_ref, out_ref):
    out_ref[...] = c_ref[...]


def solution(mesh):
    assert (mesh.shape["depth"], mesh.shape["col"], mesh.shape["row"]) == (4, 4, 8)

    def local_mm(a_blk, b_blk):
        band, kblk = a_blk.shape
        sub, half_n, steps = band // 4, kblk // 2, band // SEG
        assert sum(p[0] for p in PHASES) == sub and sum(p[2] for p in PHASES) == half_n
        c_blk = pl.pallas_call(
            functools.partial(kernel, steps),
            out_shape=jax.ShapeDtypeStruct((sub, kblk), jnp.bfloat16),
            in_specs=[pl.BlockSpec(memory_space=pl.ANY)] * 2,
            out_specs=pl.BlockSpec(memory_space=pl.ANY),
            scratch_shapes=[
                pltpu.VMEM((steps, 2, sub, 8 * SEG), jnp.bfloat16),
                pltpu.VMEM((steps, 8 * SEG, half_n), jnp.bfloat16),
                pltpu.VMEM((2, sub, half_n), jnp.float32),
                pltpu.VMEM((2, sub, half_n), jnp.bfloat16),
                pltpu.SemaphoreType.DMA((B_Z2,)),
                pltpu.SemaphoreType.DMA((KINDS, SLOTS)),
                pltpu.SemaphoreType.DMA,
                pltpu.SemaphoreType.DMA,
                pltpu.SemaphoreType.DMA,
            ],
            compiler_params=pltpu.CompilerParams(collective_id=0, has_side_effects=True, vmem_limit_bytes=67043328),
            cost_estimate=pl.CostEstimate(
                flops=4 * sub * half_n * 8 * band, bytes_accessed=4 * band * kblk, transcendentals=0
            ),
            name="gather_mm",
        )(a_blk.reshape(4, sub, kblk), b_blk)
        block = pl.BlockSpec((sub // 2, kblk), lambda r: (r, 0))
        return pl.pallas_call(
            put_out, grid=(2,), out_shape=jax.ShapeDtypeStruct(c_blk.shape, c_blk.dtype), in_specs=[block], out_specs=block
        )(c_blk)

    spec_in = P("row", "col")
    spec_out = P(("row", "depth"), "col")
    return jax.shard_map(local_mm, mesh=mesh, in_specs=(spec_in, spec_in), out_specs=spec_out, check_vma=False)
```
